32 devices in a mesh: orb: 4 (over x, core), gx: 2 (over y), gyz: 4 (over z).
Axes of the slice: x: 2, y: 2, z: 4, core: 2. Of those that a mesh axis runs over, the one named last changes fastest.
Arguments:
- orbitals: float32 [2, 12, 32, 32, 128], P(None, 'orb', 'gx', 'gyz'), parts along dimension 1, may hold values from -12 to 12
- potential: float32 [32, 32, 128], P('gx', 'gyz'), may hold values from -8 to 60
Outputs:
- evolved: float32 [2, 12, 32, 32, 128], P(None, 'orb', 'gx', 'gyz'), parts along dimension 1
- residual: float32 [2, 12, 32, 32, 128], P(None, 'orb', 'gx', 'gyz'), parts along dimension 1
The draws below stay inside these ranges and needn't reach their ends.
There are 4 independent parts, one for each index of `orb`. The reference program is written for one: setup_inputs(seed, part) draws one part's arguments, and reference() takes and returns one part's arrays. A program takes and returns all parts, laid end to end along the dimension named above; an argument that names none is the same for every part. Nothing has to cross between parts.
All inputs are finite; a program needn't handle non-finite values.
Results may differ from the reference program's by a relative error of at most 0.0003.
Values sent between devices are 32-bit elements; how exact they have to be, the bound alone decides.
A program may use at most 64 MiB of HBM per device.

```python
import jax
import jax.numpy as jnp

ORB = 3
NZ = 128
ITERS = 4
NX = 32
NY = 32


def draw_orbitals(key, part):
    shape = (2, ORB, NX, NY, NZ)
    ramp = 1.0 + 2.0 * jnp.arange(NX, dtype=jnp.float32) / (NX - 1)
    envelope = ramp[None, None, :, None, None]
    values = jax.random.normal(jax.random.fold_in(key, 13), shape, jnp.float32)
    return jnp.clip(values, -4.0, 4.0) * envelope


def draw_potential(key, part):
    rough = jax.random.uniform(jax.random.fold_in(key, 21), (NX, NY, NZ), jnp.float32, -8.0, 8.0)
    ramp = 40.0 * jnp.arange(NX, dtype=jnp.float32)[:, None, None] / (NX - 1)
    return rough + ramp


def setup_inputs(seed: int = 0, part: int = 0) -> dict:
    splits = jax.random.split(jax.random.key(seed), 3)
    own_keys = jax.random.split(jax.random.fold_in(splits[2], part), 3)
    return {
        "orbitals": draw_orbitals(jax.random.fold_in(jax.random.fold_in(splits[2], part), 71), part),
        "potential": draw_potential(jax.random.fold_in(splits[2], 71), part),
    }


SPACING = 0.25
HALF_STEP = 0.05
COEFF_NEAR = 4.0 / 3.0
COEFF_FAR = -1.0 / 12.0
COEFF_SELF = -2.5


def laplace_apply(padded, potential):
    extent = (padded.shape[2] - 4, padded.shape[3] - 4, padded.shape[4] - 4)

    def window(shift_x, shift_y, shift_z):
        return padded[:, :, 2 + shift_x:2 + shift_x + extent[0], 2 + shift_y:2 + shift_y + extent[1], 2 + shift_z:2 + shift_z + extent[2]]

    center = window(0, 0, 0)
    summed = (3.0 * COEFF_SELF) * center
    for offset, weight in ((1, COEFF_NEAR), (2, COEFF_FAR)):
        summed = summed + weight * (window(offset, 0, 0) + window(-offset, 0, 0) + window(0, offset, 0) + window(0, -offset, 0) + window(0, 0, offset) + window(0, 0, -offset))
    return (-0.5 / SPACING ** 2) * summed + potential * center


def hamiltonian(vector, potential):
    padded = jnp.pad(vector, ((0, 0), (0, 0), (2, 2), (2, 2), (2, 2)))
    return laplace_apply(padded, potential)


def system(vector, applied):
    return jnp.stack([vector[0] - HALF_STEP * applied[1], vector[1] + HALF_STEP * applied[0]])


def precondition(vector, potential):
    diagonal = HALF_STEP * (3.75 / SPACING ** 2 + potential)
    divisor = 1.0 + diagonal * diagonal
    return jnp.stack([(vector[0] + diagonal * vector[1]) / divisor, (vector[1] - diagonal * vector[0]) / divisor])


def braket(left, right):
    real_part = jnp.sum(left[0] * right[0] + left[1] * right[1], axis=(1, 2, 3))
    imag_part = jnp.sum(left[0] * right[1] - left[1] * right[0], axis=(1, 2, 3))
    return real_part, imag_part


def times_complex(first, second):
    return (first[0] * second[0] - first[1] * second[1], first[0] * second[1] + first[1] * second[0])


def divide_complex(first, second):
    modulus = second[0] * second[0] + second[1] * second[1]
    return ((first[0] * second[0] + first[1] * second[1]) / modulus, (first[1] * second[0] - first[0] * second[1]) / modulus)


def scale_complex(coeff, vector):
    real_coef = coeff[0][:, None, None, None]
    imag_coef = coeff[1][:, None, None, None]
    return jnp.stack([real_coef * vector[0] - imag_coef * vector[1], real_coef * vector[1] + imag_coef * vector[0]])


def reference(orbitals, potential):
    h_orbitals = hamiltonian(orbitals, potential)
    residual = jnp.stack([2.0 * HALF_STEP * h_orbitals[1], -2.0 * HALF_STEP * h_orbitals[0]])
    evolved = orbitals
    shadow = residual
    direction = residual
    rho_now = braket(shadow, residual)
    for iteration in range(ITERS):
        dir_hat = precondition(direction, potential)
        image = system(dir_hat, hamiltonian(dir_hat, potential))
        alpha_step = divide_complex(rho_now, braket(shadow, image))
        half_step = residual - scale_complex(alpha_step, image)
        half_hat = precondition(half_step, potential)
        second = system(half_hat, hamiltonian(half_hat, potential))
        cross = braket(second, half_step)
        norm_second = jnp.sum(second * second, axis=(0, 2, 3, 4))
        omega_step = (cross[0] / norm_second, cross[1] / norm_second)
        evolved = evolved + scale_complex(alpha_step, dir_hat) + scale_complex(omega_step, half_hat)
        residual = half_step - scale_complex(omega_step, second)
        if iteration + 1 < ITERS:
            rho_next = braket(shadow, residual)
            beta_step = times_complex(divide_complex(rho_next, rho_now), divide_complex(alpha_step, omega_step))
            direction = residual + scale_complex(beta_step, direction - scale_complex(omega_step, image))
            rho_now = rho_next
    return evolved, residual
```

```python
import functools

import jax
import jax.numpy as jnp
from jax import lax
from jax.experimental import pallas as pl
from jax.experimental.pallas import tpu as pltpu
from jax.sharding import PartitionSpec as P

ITERS = 4


SPACING = 0.25
HALF_STEP = 0.05
COEFF_NEAR = 4.0 / 3.0
COEFF_FAR = -1.0 / 12.0
COEFF_SELF = -2.5


def with_halo(array, sides, width):
    for axis, dim in sides:
        size, length = (lax.axis_size(axis), array.shape[dim])
        up = [(i, (i + 1) % size) for i in range(size - 1)]
        down = [(j, i) for i, j in up]
        last = lax.slice_in_dim(array, length - width, length, axis=dim)
        leading = lax.slice_in_dim(array, 0, width, axis=dim)
        before = lax.ppermute(last, axis, up)
        after = lax.ppermute(leading, axis, down)
        array = jnp.concatenate([before, array, after], axis=dim)
    return array


def laplace_apply(padded, potential):
    extent = (padded.shape[2] - 4, padded.shape[3] - 4, padded.shape[4] - 4)

    def window(shift_x, shift_y, shift_z):
        return padded[
            :,
            :,
            2 + shift_x : 2 + shift_x + extent[0],
            2 + shift_y : 2 + shift_y + extent[1],
            2 + shift_z : 2 + shift_z + extent[2],
        ]

    center = window(0, 0, 0)
    summed = 3.0 * COEFF_SELF * center
    for offset, weight in ((1, COEFF_NEAR), (2, COEFF_FAR)):
        summed = summed + weight * (
            window(offset, 0, 0)
            + window(-offset, 0, 0)
            + window(0, offset, 0)
            + window(0, -offset, 0)
            + window(0, 0, offset)
            + window(0, 0, -offset)
        )
    return -0.5 / SPACING**2 * summed + potential * center


def pad_depth(vector):
    return jnp.pad(vector, ((0, 0), (0, 0), (0, 0), (0, 0), (2, 2)))


def system(vector, applied):
    return jnp.stack([vector[0] - HALF_STEP * applied[1], vector[1] + HALF_STEP * applied[0]])


def precondition(vector, potential):
    diagonal = HALF_STEP * (3.75 / SPACING**2 + potential)
    divisor = 1.0 + diagonal * diagonal
    return jnp.stack(
        [(vector[0] + diagonal * vector[1]) / divisor, (vector[1] - diagonal * vector[0]) / divisor]
    )


def braket(left, right):
    real_part = jnp.sum(left[0] * right[0] + left[1] * right[1], axis=(1, 2, 3))
    imag_part = jnp.sum(left[0] * right[1] - left[1] * right[0], axis=(1, 2, 3))
    return (real_part, imag_part)


def times_complex(first, second):
    return (
        first[0] * second[0] - first[1] * second[1],
        first[0] * second[1] + first[1] * second[0],
    )


def divide_complex(first, second):
    modulus = second[0] * second[0] + second[1] * second[1]
    return (
        (first[0] * second[0] + first[1] * second[1]) / modulus,
        (first[1] * second[0] - first[0] * second[1]) / modulus,
    )


def scale_complex(coeff, vector):
    real_coef = coeff[0][:, None, None, None]
    imag_coef = coeff[1][:, None, None, None]
    return jnp.stack(
        [
            real_coef * vector[0] - imag_coef * vector[1],
            real_coef * vector[1] + imag_coef * vector[0],
        ]
    )


def shards(orbitals, potential):

    def apply_shallow(vector):
        padded = with_halo(vector, (("gx", 2), ("gyz", 3)), 2)
        return laplace_apply(pad_depth(padded), potential)

    h_orbitals = apply_shallow(orbitals)
    residual = jnp.stack([2.0 * HALF_STEP * h_orbitals[1], -2.0 * HALF_STEP * h_orbitals[0]])
    evolved = orbitals
    shadow = residual
    direction = residual
    rho_now = lax.psum(braket(shadow, residual), ("gx", "gyz"))
    for iteration in range(ITERS):
        dir_hat = precondition(direction, potential)
        image = system(dir_hat, apply_shallow(dir_hat))
        alpha_step = divide_complex(rho_now, lax.psum(braket(shadow, image), ("gx", "gyz")))
        half_step = residual - scale_complex(alpha_step, image)
        half_hat = precondition(half_step, potential)
        second = system(half_hat, apply_shallow(half_hat))
        cross_local = braket(second, half_step)
        norm_local = jnp.sum(second * second, axis=(0, 2, 3, 4))
        shadow_half = braket(shadow, half_step)
        shadow_second = braket(shadow, second)
        summed = lax.psum(
            (
                cross_local[0],
                cross_local[1],
                norm_local,
                shadow_half[0],
                shadow_half[1],
                shadow_second[0],
                shadow_second[1],
            ),
            ("gx", "gyz"),
        )
        cross_real, cross_imag, norm_second = (summed[0], summed[1], summed[2])
        omega_step = (cross_real / norm_second, cross_imag / norm_second)
        evolved = evolved + scale_complex(alpha_step, dir_hat) + scale_complex(omega_step, half_hat)
        residual = half_step - scale_complex(omega_step, second)
        if iteration + 1 < ITERS:
            along_second = times_complex(omega_step, (summed[5], summed[6]))
            rho_next = (summed[3] - along_second[0], summed[4] - along_second[1])
            beta_step = times_complex(
                divide_complex(rho_next, rho_now), divide_complex(alpha_step, omega_step)
            )
            direction = residual + scale_complex(
                beta_step, direction - scale_complex(omega_step, image)
            )
            rho_now = rho_next
    return (evolved, residual)


LEAD = 8
FIELD_BUDGET = 1 << 20
NEAR = -0.5 / SPACING**2 * COEFF_NEAR * HALF_STEP
FAR = -0.5 / SPACING**2 * COEFF_FAR * HALF_STEP


def owner_of(orb, j, size_x, size_y):
    odd = orb % 2
    turn = j // size_x
    return j % size_x, (size_y + size_y // 2 - 1 + odd + turn * (1 - 2 * odd)) % size_y


def solve_kernel(
    sizes,
    orb_ref,
    pot_ref,
    evolved_ref,
    residual_ref,
    field,
    hat_a,
    hat_b,
    shadow,
    resid,
    direction,
    image,
    second,
    pot,
    quot,
    quot_d,
    send_orb,
    recv_orb,
    send_pot,
    recv_pot,
    send_out,
    recv_out,
    local_sem,
):
    size_x, size_y = sizes
    count, bx, by, nz = orb_ref.shape[1:]
    nx, ny = (size_x * bx, size_y * by)
    orb, gx, gy = (lax.axis_index("orb"), lax.axis_index("gx"), lax.axis_index("gyz"))
    me = gx * size_y + gy
    devices = size_x * size_y
    owners = []
    for j in range(count):
        ox, oy = owner_of(orb, j, size_x, size_y)
        owners.append((ox, oy, jnp.logical_and(ox == gx, oy == gy)))
    mine = owners[0][2]
    for j in range(1, count):
        mine = jnp.logical_or(mine, owners[j][2])

    barrier = pltpu.get_barrier_semaphore()
    for dev in range(devices):
        @pl.when(me != dev)
        def _():
            pl.semaphore_signal(
                barrier,
                inc=1,
                device_id={"gx": dev // size_y, "gyz": dev % size_y},
                device_id_type=pl.DeviceIdType.MESH,
            )

    @pl.when(mine)
    def _():
        for ref in (field, hat_a, hat_b):
            edge = jnp.zeros((2, 2, ny + 2 * LEAD, nz), jnp.float32)
            ref[:, 0:2] = edge
            ref[:, nx + 2 : nx + 4] = edge

            def clear(x, carry):
                side = jnp.zeros((2, LEAD, nz), jnp.float32)
                ref[:, x + 2, 0:LEAD] = side
                ref[:, x + 2, LEAD + ny : 2 * LEAD + ny] = side
                return carry

            lax.fori_loop(0, nx, clear, 0)

    pl.semaphore_wait(barrier, devices - 1)

    def spot(ref, x_block, y_block):
        return ref.at[:, pl.ds(2 + x_block * bx, bx), pl.ds(LEAD + y_block * by, by), :]

    def pot_spot(ref, x_block, y_block):
        return ref.at[pl.ds(x_block * bx, bx), pl.ds(y_block * by, by), :]

    def inner_spot(ref, x_block, y_block):
        return ref.at[:, pl.ds(x_block * bx, bx), pl.ds(y_block * by, by), :]

    def remote(src, dst, send, recv, x, y):
        return pltpu.make_async_remote_copy(
            src_ref=src,
            dst_ref=dst,
            send_sem=send,
            recv_sem=recv,
            device_id={"gx": x, "gyz": y},
            device_id_type=pl.DeviceIdType.MESH,
        )

    def gather_copies(j):
        ox, oy, own = owners[j]
        return (
            remote(orb_ref.at[:, j], spot(field, gx, gy), send_orb.at[j], recv_orb.at[me], ox, oy),
            remote(pot_ref, pot_spot(pot, gx, gy), send_pot.at[j], recv_pot.at[me], ox, oy),
        )

    def local_copies(j):
        return (
            pltpu.make_async_copy(orb_ref.at[:, j], spot(field, gx, gy), local_sem.at[0]),
            pltpu.make_async_copy(pot_ref, pot_spot(pot, gx, gy), local_sem.at[1]),
        )

    for j in range(count):
        own = owners[j][2]

        @pl.when(jnp.logical_not(own))
        def _():
            for copy in gather_copies(j):
                copy.start()

        @pl.when(own)
        def _():
            for copy in local_copies(j):
                copy.start()

    lane = lax.broadcasted_iota(jnp.int32, (ny, nz), 1)

    def neighbours(ref, part, x):
        def at(dx, dy):
            return ref[part, x + 2 + dx, LEAD + dy : LEAD + dy + ny, :]

        center = at(0, 0)
        near = (at(1, 0) + at(-1, 0)) + (at(0, 1) + at(0, -1))
        far = (at(2, 0) + at(-2, 0)) + (at(0, 2) + at(0, -2))
        near = near + (
            jnp.where(lane < 1, 0.0, pltpu.roll(center, 1, 1))
            + jnp.where(lane >= nz - 1, 0.0, pltpu.roll(center, nz - 1, 1))
        )
        far = far + (
            jnp.where(lane < 2, 0.0, pltpu.roll(center, 2, 1))
            + jnp.where(lane >= nz - 2, 0.0, pltpu.roll(center, nz - 2, 1))
        )
        return NEAR * near + FAR * far, center

    def fold(value):
        return jnp.sum(value.reshape(ny // 8, 8, nz), axis=0)

    def total(value):
        return jnp.sum(value, keepdims=True)

    zero = jnp.zeros((8, nz), jnp.float32)
    rows = slice(LEAD, LEAD + ny)

    def set_hat(hat, x, re, im):
        q, qd = (quot[x], quot_d[x])
        hat[0, x + 2, rows, :] = q * re + qd * im
        hat[1, x + 2, rows, :] = q * im - qd * re

    def start_plane(x, rho):
        d = HALF_STEP * (-1.5 * COEFF_SELF / SPACING**2 + pot[x])
        q = 1.0 / (1.0 + d * d)
        quot[x] = q
        quot_d[x] = q * d
        off_re, re = neighbours(field, 0, x)
        off_im, im = neighbours(field, 1, x)
        r_re = 2.0 * (off_im + d * im)
        r_im = -2.0 * (off_re + d * re)
        for ref in (shadow, resid, direction):
            ref[0, x] = r_re
            ref[1, x] = r_im
        set_hat(hat_a, x, r_re, r_im)
        return rho + fold(r_re * r_re + r_im * r_im)

    def image_plane(x, sums):
        off_re, _ = neighbours(hat_a, 0, x)
        off_im, _ = neighbours(hat_a, 1, x)
        i_re = direction[0, x] - off_im
        i_im = direction[1, x] + off_re
        image[0, x] = i_re
        image[1, x] = i_im
        s_re, s_im = (shadow[0, x], shadow[1, x])
        return (
            sums[0] + fold(s_re * i_re + s_im * i_im),
            sums[1] + fold(s_re * i_im - s_im * i_re),
        )

    def half_plane(alpha, x, sums):
        i_re, i_im = (image[0, x], image[1, x])
        h_re = resid[0, x] - (alpha[0] * i_re - alpha[1] * i_im)
        h_im = resid[1, x] - (alpha[0] * i_im + alpha[1] * i_re)
        resid[0, x] = h_re
        resid[1, x] = h_im
        set_hat(hat_b, x, h_re, h_im)
        s_re, s_im = (shadow[0, x], shadow[1, x])
        return (
            sums[0] + fold(s_re * h_re + s_im * h_im),
            sums[1] + fold(s_re * h_im - s_im * h_re),
        )

    def second_plane(x, sums):
        off_re, _ = neighbours(hat_b, 0, x)
        off_im, _ = neighbours(hat_b, 1, x)
        h_re, h_im = (resid[0, x], resid[1, x])
        t_re = h_re - off_im
        t_im = h_im + off_re
        second[0, x] = t_re
        second[1, x] = t_im
        s_re, s_im = (shadow[0, x], shadow[1, x])
        return (
            sums[0] + fold(t_re * h_re + t_im * h_im),
            sums[1] + fold(t_re * h_im - t_im * h_re),
            sums[2] + fold(t_re * t_re + t_im * t_im),
            sums[3] + fold(s_re * t_re + s_im * t_im),
            sums[4] + fold(s_re * t_im - s_im * t_re),
        )

    def update_plane(alpha, omega, x):
        a_re, a_im = (hat_a[0, x + 2, rows, :], hat_a[1, x + 2, rows, :])
        b_re, b_im = (hat_b[0, x + 2, rows, :], hat_b[1, x + 2, rows, :])
        t_re, t_im = (second[0, x], second[1, x])
        field[0, x + 2, rows, :] = (
            field[0, x + 2, rows, :]
            + (alpha[0] * a_re - alpha[1] * a_im)
            + (omega[0] * b_re - omega[1] * b_im)
        )
        field[1, x + 2, rows, :] = (
            field[1, x + 2, rows, :]
            + (alpha[0] * a_im + alpha[1] * a_re)
            + (omega[0] * b_im + omega[1] * b_re)
        )
        r_re = resid[0, x] - (omega[0] * t_re - omega[1] * t_im)
        r_im = resid[1, x] - (omega[0] * t_im + omega[1] * t_re)
        resid[0, x] = r_re
        resid[1, x] = r_im
        return r_re, r_im

    def next_plane(alpha, omega, beta, x, carry):
        r_re, r_im = update_plane(alpha, omega, x)
        i_re, i_im = (image[0, x], image[1, x])
        u_re = direction[0, x] - (omega[0] * i_re - omega[1] * i_im)
        u_im = direction[1, x] - (omega[0] * i_im + omega[1] * i_re)
        d_re = r_re + (beta[0] * u_re - beta[1] * u_im)
        d_im = r_im + (beta[0] * u_im + beta[1] * u_re)
        direction[0, x] = d_re
        direction[1, x] = d_im
        set_hat(hat_a, x, d_re, d_im)
        return carry

    def out_copies(j, x, y):
        slot = x * size_y + y
        return (
            remote(
                spot(field, x, y), evolved_ref.at[:, j], send_out.at[0, slot], recv_out.at[0, j], x, y
            ),
            remote(
                inner_spot(resid, x, y),
                residual_ref.at[:, j],
                send_out.at[1, slot],
                recv_out.at[1, j],
                x,
                y,
            ),
        )

    def out_local(j):
        return (
            pltpu.make_async_copy(spot(field, gx, gy), evolved_ref.at[:, j], local_sem.at[0]),
            pltpu.make_async_copy(inner_spot(resid, gx, gy), residual_ref.at[:, j], local_sem.at[1]),
        )

    def each_out(x, act):
        for j in range(count):
            for y in range(size_y):
                other = jnp.logical_or(gx != x, gy != y)

                @pl.when(jnp.logical_and(owners[j][2], other))
                def _():
                    for copy in out_copies(j, x, y):
                        act(copy)

                @pl.when(jnp.logical_and(owners[j][2], jnp.logical_not(other)))
                def _():
                    for copy in out_local(j):
                        if act is begin:
                            copy.start()
                        else:
                            copy.wait()

    def begin(copy):
        copy.start()

    def finish(copy):
        copy.wait_send()

    @pl.when(mine)
    def _():
        for dev in range(devices):
            x, y = (dev // size_y, dev % size_y)

            @pl.when(me != dev)
            def _():
                remote(
                    orb_ref.at[:, 0], spot(field, x, y), send_orb.at[0], recv_orb.at[dev], x, y
                ).wait_recv()
                remote(
                    pot_ref, pot_spot(pot, x, y), send_pot.at[0], recv_pot.at[dev], x, y
                ).wait_recv()

        for copy in local_copies(0):
            copy.wait()

        rho_sum = lax.fori_loop(0, nx, start_plane, zero)
        rho = (total(rho_sum), jnp.zeros((1, 1), jnp.float32))
        for iteration in range(ITERS):
            sums = lax.fori_loop(0, nx, image_plane, (zero, zero))
            alpha = divide_complex(rho, (total(sums[0]), total(sums[1])))
            held = lax.fori_loop(0, nx, functools.partial(half_plane, alpha), (zero, zero))
            sums = lax.fori_loop(0, nx, second_plane, (zero,) * 5)
            norm = total(sums[2])
            omega = (total(sums[0]) / norm, total(sums[1]) / norm)
            if iteration + 1 < ITERS:
                along = times_complex(omega, (total(sums[3]), total(sums[4])))
                rho_next = (total(held[0]) - along[0], total(held[1]) - along[1])
                beta = times_complex(divide_complex(rho_next, rho), divide_complex(alpha, omega))
                rho = rho_next
                lax.fori_loop(0, nx, functools.partial(next_plane, alpha, omega, beta), 0)

        def last_plane(x, carry):
            update_plane(alpha, omega, x)
            return carry

        for x in range(size_x):
            lax.fori_loop(x * bx, (x + 1) * bx, last_plane, 0)
            each_out(x, begin)
        for x in range(size_x):
            each_out(x, finish)

    for j in range(count):
        @pl.when(jnp.logical_not(owners[j][2]))
        def _():
            for copy in gather_copies(j):
                copy.wait_send()
            for copy in out_copies(j, 0, 0):
                copy.wait_recv()


def gathered(sizes, orbitals, potential):
    size_x, size_y = sizes
    _, count, bx, by, nz = orbitals.shape
    nx, ny = (size_x * bx, size_y * by)
    padded = pltpu.VMEM((2, nx + 4, ny + 2 * LEAD, nz), jnp.float32)
    plain = pltpu.VMEM((2, nx, ny, nz), jnp.float32)
    scalar = pltpu.VMEM((nx, ny, nz), jnp.float32)
    dma = pltpu.SemaphoreType.DMA
    devices = size_x * size_y
    shape = jax.ShapeDtypeStruct(orbitals.shape, jnp.float32)
    return pl.pallas_call(
        functools.partial(solve_kernel, sizes),
        out_shape=(shape, shape),
        in_specs=[pl.BlockSpec(memory_space=pltpu.VMEM)] * 2,
        out_specs=(pl.BlockSpec(memory_space=pltpu.VMEM),) * 2,
        scratch_shapes=[padded] * 3
        + [plain] * 5
        + [scalar] * 3
        + [
            dma((count,)),
            dma((devices,)),
            dma((count,)),
            dma((devices,)),
            dma((2, devices)),
            dma((2, count)),
            dma((2,)),
        ],
        compiler_params=pltpu.CompilerParams(
            collective_id=0, has_side_effects=True, vmem_limit_bytes=48 * 1024 * 1024
        ),
    )(orbitals, potential)


def step(sizes, orbitals, potential):
    _, count, bx, by, nz = orbitals.shape
    devices = sizes[0] * sizes[1]
    fits = 8 * devices * bx * by * nz <= FIELD_BUDGET
    if fits and count <= devices and by % 8 == 0 and nz % 128 == 0:
        return gathered(sizes, orbitals, potential)
    return shards(orbitals, potential)


def solution(mesh):
    sizes = (mesh.shape["gx"], mesh.shape["gyz"])
    return jax.shard_map(
        functools.partial(step, sizes),
        mesh=mesh,
        in_specs=(P(None, "orb", "gx", "gyz", None), P("gx", "gyz", None)),
        out_specs=(P(None, "orb", "gx", "gyz", None), P(None, "orb", "gx", "gyz", None)),
        check_vma=False,
    )
```

```python
import functools

import jax
import jax.numpy as jnp
from jax import lax
from jax.experimental import pallas as pl
from jax.experimental.pallas import tpu as pltpu
from jax.sharding import PartitionSpec as P

ITERS = 4


SPACING = 0.25
HALF_STEP = 0.05
COEFF_NEAR = 4.0 / 3.0
COEFF_FAR = -1.0 / 12.0
COEFF_SELF = -2.5


def with_halo(array, sides, width):
    for axis, dim in sides:
        size, length = (lax.axis_size(axis), array.shape[dim])
        up = [(i, (i + 1) % size) for i in range(size - 1)]
        down = [(j, i) for i, j in up]
        last = lax.slice_in_dim(array, length - width, length, axis=dim)
        leading = lax.slice_in_dim(array, 0, width, axis=dim)
        before = lax.ppermute(last, axis, up)
        after = lax.ppermute(leading, axis, down)
        array = jnp.concatenate([before, array, after], axis=dim)
    return array


def laplace_apply(padded, potential):
    extent = (padded.shape[2] - 4, padded.shape[3] - 4, padded.shape[4] - 4)

    def window(shift_x, shift_y, shift_z):
        return padded[
            :,
            :,
            2 + shift_x : 2 + shift_x + extent[0],
            2 + shift_y : 2 + shift_y + extent[1],
            2 + shift_z : 2 + shift_z + extent[2],
        ]

    center = window(0, 0, 0)
    summed = 3.0 * COEFF_SELF * center
    for offset, weight in ((1, COEFF_NEAR), (2, COEFF_FAR)):
        summed = summed + weight * (
            window(offset, 0, 0)
            + window(-offset, 0, 0)
            + window(0, offset, 0)
            + window(0, -offset, 0)
            + window(0, 0, offset)
            + window(0, 0, -offset)
        )
    return -0.5 / SPACING**2 * summed + potential * center


def pad_depth(vector):
    return jnp.pad(vector, ((0, 0), (0, 0), (0, 0), (0, 0), (2, 2)))


def system(vector, applied):
    return jnp.stack([vector[0] - HALF_STEP * applied[1], vector[1] + HALF_STEP * applied[0]])


def precondition(vector, potential):
    diagonal = HALF_STEP * (3.75 / SPACING**2 + potential)
    divisor = 1.0 + diagonal * diagonal
    return jnp.stack(
        [(vector[0] + diagonal * vector[1]) / divisor, (vector[1] - diagonal * vector[0]) / divisor]
    )


def braket(left, right):
    real_part = jnp.sum(left[0] * right[0] + left[1] * right[1], axis=(1, 2, 3))
    imag_part = jnp.sum(left[0] * right[1] - left[1] * right[0], axis=(1, 2, 3))
    return (real_part, imag_part)


def times_complex(first, second):
    return (
        first[0] * second[0] - first[1] * second[1],
        first[0] * second[1] + first[1] * second[0],
    )


def divide_complex(first, second):
    modulus = second[0] * second[0] + second[1] * second[1]
    return (
        (first[0] * second[0] + first[1] * second[1]) / modulus,
        (first[1] * second[0] - first[0] * second[1]) / modulus,
    )


def scale_complex(coeff, vector):
    real_coef = coeff[0][:, None, None, None]
    imag_coef = coeff[1][:, None, None, None]
    return jnp.stack(
        [
            real_coef * vector[0] - imag_coef * vector[1],
            real_coef * vector[1] + imag_coef * vector[0],
        ]
    )


def shards(orbitals, potential):

    def apply_shallow(vector):
        padded = with_halo(vector, (("gx", 2), ("gyz", 3)), 2)
        return laplace_apply(pad_depth(padded), potential)

    h_orbitals = apply_shallow(orbitals)
    residual = jnp.stack([2.0 * HALF_STEP * h_orbitals[1], -2.0 * HALF_STEP * h_orbitals[0]])
    evolved = orbitals
    shadow = residual
    direction = residual
    rho_now = lax.psum(braket(shadow, residual), ("gx", "gyz"))
    for iteration in range(ITERS):
        dir_hat = precondition(direction, potential)
        image = system(dir_hat, apply_shallow(dir_hat))
        alpha_step = divide_complex(rho_now, lax.psum(braket(shadow, image), ("gx", "gyz")))
        half_step = residual - scale_complex(alpha_step, image)
        half_hat = precondition(half_step, potential)
        second = system(half_hat, apply_shallow(half_hat))
        cross_local = braket(second, half_step)
        norm_local = jnp.sum(second * second, axis=(0, 2, 3, 4))
        shadow_half = braket(shadow, half_step)
        shadow_second = braket(shadow, second)
        summed = lax.psum(
            (
                cross_local[0],
                cross_local[1],
                norm_local,
                shadow_half[0],
                shadow_half[1],
                shadow_second[0],
                shadow_second[1],
            ),
            ("gx", "gyz"),
        )
        cross_real, cross_imag, norm_second = (summed[0], summed[1], summed[2])
        omega_step = (cross_real / norm_second, cross_imag / norm_second)
        evolved = evolved + scale_complex(alpha_step, dir_hat) + scale_complex(omega_step, half_hat)
        residual = half_step - scale_complex(omega_step, second)
        if iteration + 1 < ITERS:
            along_second = times_complex(omega_step, (summed[5], summed[6]))
            rho_next = (summed[3] - along_second[0], summed[4] - along_second[1])
            beta_step = times_complex(
                divide_complex(rho_next, rho_now), divide_complex(alpha_step, omega_step)
            )
            direction = residual + scale_complex(
                beta_step, direction - scale_complex(omega_step, image)
            )
            rho_now = rho_next
    return (evolved, residual)


UNROLL = 8
LEAD = 8
FIELD_BUDGET = 1 << 20
NEAR = -0.5 / SPACING**2 * COEFF_NEAR * HALF_STEP
FAR = -0.5 / SPACING**2 * COEFF_FAR * HALF_STEP


def owner_of(odd, j, size_x, size_y):
    middle = size_y // 2
    if odd:
        return (1 + j // size_x) % size_x, (middle + j) % size_y
    return j % size_x, (size_y + middle - 1 + j // size_x) % size_y


def sweep(start, stop, plane, carry):
    width = UNROLL if (stop - start) % UNROLL == 0 else 1

    def group(i, carry):
        for k in range(width):
            carry = plane(start + i * width + k, carry)
        return carry

    return lax.fori_loop(0, (stop - start) // width, group, carry)


def solve_kernel(
    sizes,
    orb_ref,
    pot_ref,
    evolved_ref,
    residual_ref,
    field,
    hat_a,
    hat_b,
    shadow,
    resid,
    direction,
    image,
    second,
    pot,
    quot,
    quot_d,
    send_orb,
    recv_orb,
    send_pot,
    recv_pot,
    send_out,
    recv_out,
    local_sem,
):
    size_x, size_y = sizes
    count, bx, by, nz = orb_ref.shape[1:]
    nx, ny = (size_x * bx, size_y * by)
    orb, gx, gy = (lax.axis_index("orb"), lax.axis_index("gx"), lax.axis_index("gyz"))
    me = gx * size_y + gy
    devices = size_x * size_y
    owners = []
    for j in range(count):
        even, odd = (owner_of(parity, j, size_x, size_y) for parity in (0, 1))
        ox = jnp.where(orb % 2 == 1, odd[0], even[0])
        oy = jnp.where(orb % 2 == 1, odd[1], even[1])
        owners.append((ox, oy, jnp.logical_and(ox == gx, oy == gy)))
    mine = owners[0][2]
    for j in range(1, count):
        mine = jnp.logical_or(mine, owners[j][2])

    barrier = pltpu.get_barrier_semaphore()
    for dev in range(devices):
        @pl.when(me != dev)
        def _():
            pl.semaphore_signal(
                barrier,
                inc=1,
                device_id={"gx": dev // size_y, "gyz": dev % size_y},
                device_id_type=pl.DeviceIdType.MESH,
            )

    @pl.when(mine)
    def _():
        for ref in (field, hat_a, hat_b):
            edge = jnp.zeros((2, 2, ny + 2 * LEAD, nz), jnp.float32)
            ref[:, 0:2] = edge
            ref[:, nx + 2 : nx + 4] = edge

            def clear(x, carry):
                side = jnp.zeros((2, LEAD, nz), jnp.float32)
                ref[:, x + 2, 0:LEAD] = side
                ref[:, x + 2, LEAD + ny : 2 * LEAD + ny] = side
                return carry

            lax.fori_loop(0, nx, clear, 0)

    pl.semaphore_wait(barrier, devices - 1)

    def spot(ref, x_block, y_block):
        return ref.at[:, pl.ds(2 + x_block * bx, bx), pl.ds(LEAD + y_block * by, by), :]

    def pot_spot(ref, x_block, y_block):
        return ref.at[pl.ds(x_block * bx, bx), pl.ds(y_block * by, by), :]

    def inner_spot(ref, x_block, y_block):
        return ref.at[:, pl.ds(x_block * bx, bx), pl.ds(y_block * by, by), :]

    def remote(src, dst, send, recv, x, y):
        return pltpu.make_async_remote_copy(
            src_ref=src,
            dst_ref=dst,
            send_sem=send,
            recv_sem=recv,
            device_id={"gx": x, "gyz": y},
            device_id_type=pl.DeviceIdType.MESH,
        )

    def gather_copies(j):
        ox, oy, own = owners[j]
        return (
            remote(orb_ref.at[:, j], spot(field, gx, gy), send_orb.at[j], recv_orb.at[me], ox, oy),
            remote(pot_ref, pot_spot(pot, gx, gy), send_pot.at[j], recv_pot.at[me], ox, oy),
        )

    def local_copies(j):
        return (
            pltpu.make_async_copy(orb_ref.at[:, j], spot(field, gx, gy), local_sem.at[0]),
            pltpu.make_async_copy(pot_ref, pot_spot(pot, gx, gy), local_sem.at[1]),
        )

    for j in range(count):
        own = owners[j][2]

        @pl.when(jnp.logical_not(own))
        def _():
            for copy in gather_copies(j):
                copy.start()

        @pl.when(own)
        def _():
            for copy in local_copies(j):
                copy.start()

    lane = lax.broadcasted_iota(jnp.int32, (ny, nz), 1)

    def neighbours(ref, part, x):
        def at(dx, dy):
            return ref[part, x + 2 + dx, LEAD + dy : LEAD + dy + ny, :]

        center = at(0, 0)
        near = (at(1, 0) + at(-1, 0)) + (at(0, 1) + at(0, -1))
        far = (at(2, 0) + at(-2, 0)) + (at(0, 2) + at(0, -2))
        near = near + (
            jnp.where(lane < 1, 0.0, pltpu.roll(center, 1, 1))
            + jnp.where(lane >= nz - 1, 0.0, pltpu.roll(center, nz - 1, 1))
        )
        far = far + (
            jnp.where(lane < 2, 0.0, pltpu.roll(center, 2, 1))
            + jnp.where(lane >= nz - 2, 0.0, pltpu.roll(center, nz - 2, 1))
        )
        return NEAR * near + FAR * far, center

    def fold(value):
        return jnp.sum(value.reshape(ny // 8, 8, nz), axis=0)

    def total(value):
        return jnp.sum(value, keepdims=True)

    zero = jnp.zeros((8, nz), jnp.float32)
    rows = slice(LEAD, LEAD + ny)

    def set_hat(hat, x, re, im):
        q, qd = (quot[x], quot_d[x])
        hat[0, x + 2, rows, :] = q * re + qd * im
        hat[1, x + 2, rows, :] = q * im - qd * re

    def start_plane(x, rho):
        d = HALF_STEP * (-1.5 * COEFF_SELF / SPACING**2 + pot[x])
        q = 1.0 / (1.0 + d * d)
        quot[x] = q
        quot_d[x] = q * d
        off_re, re = neighbours(field, 0, x)
        off_im, im = neighbours(field, 1, x)
        r_re = 2.0 * (off_im + d * im)
        r_im = -2.0 * (off_re + d * re)
        for ref in (shadow, resid, direction):
            ref[0, x] = r_re
            ref[1, x] = r_im
        set_hat(hat_a, x, r_re, r_im)
        return rho + fold(r_re * r_re + r_im * r_im)

    def image_plane(x, sums):
        off_re, _ = neighbours(hat_a, 0, x)
        off_im, _ = neighbours(hat_a, 1, x)
        i_re = direction[0, x] - off_im
        i_im = direction[1, x] + off_re
        image[0, x] = i_re
        image[1, x] = i_im
        s_re, s_im = (shadow[0, x], shadow[1, x])
        return (
            sums[0] + fold(s_re * i_re + s_im * i_im),
            sums[1] + fold(s_re * i_im - s_im * i_re),
        )

    def half_plane(alpha, x, sums):
        i_re, i_im = (image[0, x], image[1, x])
        h_re = resid[0, x] - (alpha[0] * i_re - alpha[1] * i_im)
        h_im = resid[1, x] - (alpha[0] * i_im + alpha[1] * i_re)
        resid[0, x] = h_re
        resid[1, x] = h_im
        set_hat(hat_b, x, h_re, h_im)
        s_re, s_im = (shadow[0, x], shadow[1, x])
        return (
            sums[0] + fold(s_re * h_re + s_im * h_im),
            sums[1] + fold(s_re * h_im - s_im * h_re),
        )

    def second_plane(x, sums):
        off_re, _ = neighbours(hat_b, 0, x)
        off_im, _ = neighbours(hat_b, 1, x)
        h_re, h_im = (resid[0, x], resid[1, x])
        t_re = h_re - off_im
        t_im = h_im + off_re
        second[0, x] = t_re
        second[1, x] = t_im
        s_re, s_im = (shadow[0, x], shadow[1, x])
        return (
            sums[0] + fold(t_re * h_re + t_im * h_im),
            sums[1] + fold(t_re * h_im - t_im * h_re),
            sums[2] + fold(t_re * t_re + t_im * t_im),
            sums[3] + fold(s_re * t_re + s_im * t_im),
            sums[4] + fold(s_re * t_im - s_im * t_re),
        )

    def update_plane(alpha, omega, x):
        a_re, a_im = (hat_a[0, x + 2, rows, :], hat_a[1, x + 2, rows, :])
        b_re, b_im = (hat_b[0, x + 2, rows, :], hat_b[1, x + 2, rows, :])
        t_re, t_im = (second[0, x], second[1, x])
        field[0, x + 2, rows, :] = (
            field[0, x + 2, rows, :]
            + (alpha[0] * a_re - alpha[1] * a_im)
            + (omega[0] * b_re - omega[1] * b_im)
        )
        field[1, x + 2, rows, :] = (
            field[1, x + 2, rows, :]
            + (alpha[0] * a_im + alpha[1] * a_re)
            + (omega[0] * b_im + omega[1] * b_re)
        )
        r_re = resid[0, x] - (omega[0] * t_re - omega[1] * t_im)
        r_im = resid[1, x] - (omega[0] * t_im + omega[1] * t_re)
        resid[0, x] = r_re
        resid[1, x] = r_im
        return r_re, r_im

    def next_plane(alpha, omega, beta, x, carry):
        r_re, r_im = update_plane(alpha, omega, x)
        i_re, i_im = (image[0, x], image[1, x])
        u_re = direction[0, x] - (omega[0] * i_re - omega[1] * i_im)
        u_im = direction[1, x] - (omega[0] * i_im + omega[1] * i_re)
        d_re = r_re + (beta[0] * u_re - beta[1] * u_im)
        d_im = r_im + (beta[0] * u_im + beta[1] * u_re)
        direction[0, x] = d_re
        direction[1, x] = d_im
        set_hat(hat_a, x, d_re, d_im)
        return carry

    def out_copies(j, x, y):
        slot = x * size_y + y
        return (
            remote(
                spot(field, x, y), evolved_ref.at[:, j], send_out.at[0, slot], recv_out.at[0, j], x, y
            ),
            remote(
                inner_spot(resid, x, y),
                residual_ref.at[:, j],
                send_out.at[1, slot],
                recv_out.at[1, j],
                x,
                y,
            ),
        )

    def out_local(j):
        return (
            pltpu.make_async_copy(spot(field, gx, gy), evolved_ref.at[:, j], local_sem.at[0]),
            pltpu.make_async_copy(inner_spot(resid, gx, gy), residual_ref.at[:, j], local_sem.at[1]),
        )

    def each_out(x, act):
        for j in range(count):
            for y in range(size_y):
                other = jnp.logical_or(gx != x, gy != y)

                @pl.when(jnp.logical_and(owners[j][2], other))
                def _():
                    for copy in out_copies(j, x, y):
                        act(copy)

                @pl.when(jnp.logical_and(owners[j][2], jnp.logical_not(other)))
                def _():
                    for copy in out_local(j):
                        if act is begin:
                            copy.start()
                        else:
                            copy.wait()

    def begin(copy):
        copy.start()

    def finish(copy):
        copy.wait_send()

    @pl.when(mine)
    def _():
        for dev in range(devices):
            x, y = (dev // size_y, dev % size_y)

            @pl.when(me != dev)
            def _():
                remote(
                    orb_ref.at[:, 0], spot(field, x, y), send_orb.at[0], recv_orb.at[dev], x, y
                ).wait_recv()
                remote(
                    pot_ref, pot_spot(pot, x, y), send_pot.at[0], recv_pot.at[dev], x, y
                ).wait_recv()

        for copy in local_copies(0):
            copy.wait()

        rho_sum = sweep(0, nx, start_plane, zero)
        rho = (total(rho_sum), jnp.zeros((1, 1), jnp.float32))
        for iteration in range(ITERS):
            sums = sweep(0, nx, image_plane, (zero, zero))
            alpha = divide_complex(rho, (total(sums[0]), total(sums[1])))
            held = sweep(0, nx, functools.partial(half_plane, alpha), (zero, zero))
            sums = sweep(0, nx, second_plane, (zero,) * 5)
            norm = total(sums[2])
            omega = (total(sums[0]) / norm, total(sums[1]) / norm)
            if iteration + 1 < ITERS:
                along = times_complex(omega, (total(sums[3]), total(sums[4])))
                rho_next = (total(held[0]) - along[0], total(held[1]) - along[1])
                beta = times_complex(divide_complex(rho_next, rho), divide_complex(alpha, omega))
                rho = rho_next
                sweep(0, nx, functools.partial(next_plane, alpha, omega, beta), 0)

        def last_plane(x, carry):
            update_plane(alpha, omega, x)
            return carry

        for x in range(size_x):
            sweep(x * bx, (x + 1) * bx, last_plane, 0)
            each_out(x, begin)
        for x in range(size_x):
            each_out(x, finish)

    for j in range(count):
        @pl.when(jnp.logical_not(owners[j][2]))
        def _():
            for copy in gather_copies(j):
                copy.wait_send()
            for copy in out_copies(j, 0, 0):
                copy.wait_recv()


def gathered(sizes, orbitals, potential):
    size_x, size_y = sizes
    _, count, bx, by, nz = orbitals.shape
    nx, ny = (size_x * bx, size_y * by)
    padded = pltpu.VMEM((2, nx + 4, ny + 2 * LEAD, nz), jnp.float32)
    plain = pltpu.VMEM((2, nx, ny, nz), jnp.float32)
    scalar = pltpu.VMEM((nx, ny, nz), jnp.float32)
    dma = pltpu.SemaphoreType.DMA
    devices = size_x * size_y
    shape = jax.ShapeDtypeStruct(orbitals.shape, jnp.float32)
    return pl.pallas_call(
        functools.partial(solve_kernel, sizes),
        out_shape=(shape, shape),
        in_specs=[pl.BlockSpec(memory_space=pltpu.VMEM)] * 2,
        out_specs=(pl.BlockSpec(memory_space=pltpu.VMEM),) * 2,
        scratch_shapes=[padded] * 3
        + [plain] * 5
        + [scalar] * 3
        + [
            dma((count,)),
            dma((devices,)),
            dma((count,)),
            dma((devices,)),
            dma((2, devices)),
            dma((2, count)),
            dma((2,)),
        ],
        compiler_params=pltpu.CompilerParams(
            collective_id=0, has_side_effects=True, vmem_limit_bytes=48 * 1024 * 1024
        ),
    )(orbitals, potential)


def step(sizes, orbitals, potential):
    _, count, bx, by, nz = orbitals.shape
    devices = sizes[0] * sizes[1]
    fits = 8 * devices * bx * by * nz <= FIELD_BUDGET
    distinct = all(
        len({owner_of(parity, j, *sizes) for j in range(count)}) == count for parity in (0, 1)
    )
    if fits and distinct and by % 8 == 0 and nz % 128 == 0:
        return gathered(sizes, orbitals, potential)
    return shards(orbitals, potential)


def solution(mesh):
    sizes = (mesh.shape["gx"], mesh.shape["gyz"])
    return jax.shard_map(
        functools.partial(step, sizes),
        mesh=mesh,
        in_specs=(P(None, "orb", "gx", "gyz", None), P("gx", "gyz", None)),
        out_specs=(P(None, "orb", "gx", "gyz", None), P(None, "orb", "gx", "gyz", None)),
        check_vma=False,
    )
```
